32 devices in a mesh: tm: 32 (over z, y, x, core).
Axes of the slice: x: 2, y: 2, z: 4, core: 2. Of those that a mesh axis runs over, the one named last changes fastest.
Arguments:
- prior_mean: float32 [128], replicated, may hold values from -6 to 6
- rates: float32 [64], replicated, may hold values from 0.00390625 to 0.3
- observed: float32 [512, 64], P('tm'), may hold values from -6 to 6
- mask: int32 [512, 64], P('tm'), may hold values 0 or 1
- gains: bfloat16 [512, 128, 64], P('tm'), may hold values from -0.3 to 0.3
- smooth_gains: bfloat16 [512, 128, 128], P('tm'), may hold values from -0.1 to 1
- weights: bfloat16 [512, 64, 64], P('tm'), may hold values from -0.1 to 3.5, as said below
Outputs:
- filtered: float32 [512, 128], P('tm')
- smoothed: float32 [512, 128], P('tm')
- fit: float32 [], replicated
The draws below stay inside these ranges and needn't reach their ends.
Inputs may be any that keep to these rules, and one draw needn't show every extreme that they name: `weights`: symmetric.
All inputs are finite; a program needn't handle non-finite values. No bound on the sum of `mask` on one device may be relied on, other than what follows from the above.
Results may differ from the reference program's by a relative error of at most 0.0003.
Values sent between devices are 32-bit elements; how exact they have to be, the bound alone decides.
A program may use at most 64 MiB of HBM per device.

```python
import math
import jax
import jax.numpy as jnp
from jax import lax

SITES = 64
ORDER = 2
STATE = 128
STEPS = 512


def draw_gains(key, part):
    state = SITES * ORDER
    first, second, third = jax.random.split(jax.random.fold_in(key, 11), 3)
    site_rate = jnp.exp(jax.random.uniform(first, (SITES,), jnp.float32, math.log(1.0 / STEPS), math.log(0.1)))
    step_scale = jax.random.uniform(second, (STEPS, 1, SITES), jnp.float32, 0.5, 1.5)
    eye = jnp.eye(SITES, dtype=jnp.float32)
    pattern = jnp.concatenate([eye, 0.5 * eye], axis=0)
    noise = jax.random.normal(third, (STEPS, state, SITES), jnp.float32) * (0.2 / math.sqrt(state))
    full = (pattern[None] + jnp.clip(noise, -1.0, 1.0)) * (site_rate[None, None, :] * step_scale)
    return full.astype(jnp.bfloat16)


def draw_smooth_gains(key, part):
    state = SITES * ORDER
    first, second, third = jax.random.split(jax.random.fold_in(key, 23), 3)
    comp_rate = jnp.exp(jax.random.uniform(first, (state,), jnp.float32, math.log(1.0 / STEPS), math.log(0.1)))
    step_scale = jax.random.uniform(second, (STEPS, state), jnp.float32, 0.5, 1.5)
    keep = jnp.exp(-comp_rate[None, :] * step_scale)
    noise = jnp.clip(jax.random.normal(third, (STEPS, state, state), jnp.float32), -6.0, 6.0)
    noise = noise * (0.3 * comp_rate[None, :, None] / math.sqrt(state))
    full = noise + keep[:, :, None] * jnp.eye(state, dtype=jnp.float32)[None]
    return full.astype(jnp.bfloat16)


def draw_weights(key, part):
    first, second = jax.random.split(jax.random.fold_in(key, 37), 2)
    diag = jnp.exp(jax.random.uniform(first, (STEPS, SITES), jnp.float32, math.log(0.3), math.log(3.0)))
    noise = jnp.clip(jax.random.normal(second, (STEPS, SITES, SITES), jnp.float32), -6.0, 6.0) * (0.3 / SITES)
    sym = 0.5 * (noise + jnp.swapaxes(noise, 1, 2))
    eye = jnp.eye(SITES, dtype=jnp.float32)
    full = sym * (1.0 - eye)[None] + diag[:, :, None] * eye[None]
    return full.astype(jnp.bfloat16)


def with_ends(array, stream_key, least, largest):
    longest = array.shape.index(max(array.shape))
    spots = []
    for shift in (0, 1):
        where = [jax.random.randint(jax.random.fold_in(stream_key, axis), (), 0, length) for axis, length in enumerate(array.shape)]
        where[longest] = (where[longest] + shift) % array.shape[longest]
        spots.append(tuple(where))
    return array.at[spots[0]].set(least).at[spots[1]].set(largest)


def block_levels(stream_key, extent, cuts, low, largest):
    def one(dim, shards_of):
        steps = jax.random.uniform(jax.random.fold_in(jax.random.fold_in(stream_key, 6), dim), (shards_of,), jnp.float32, low / len(cuts), largest / len(cuts))
        return jnp.repeat(jnp.exp(steps), extent[dim] // shards_of).reshape((-1,) + (1,) * (len(extent) - dim - 1))

    level = one(*cuts[0])
    for cut in cuts[1:]:
        level = level * one(*cut)
    return level


def normal_values(stream_key, shape, scale, reach, cuts=(), kind=jnp.bfloat16):
    entries = scale * jax.random.normal(stream_key, shape, jnp.float32)
    if cuts:
        entries = entries * block_levels(stream_key, shape, cuts, -0.22, 0.18)
    return jnp.clip(entries, -reach, reach).astype(kind)


def setup_inputs(seed: int = 0) -> dict:
    key_of = jax.random.split(jax.random.key(seed), 8)
    return {
        "prior_mean": normal_values(key_of[0], (STATE,), 1.0, 6.0, (), jnp.float32),
        "rates": jnp.clip(jnp.exp(jax.random.uniform(key_of[1], (SITES,), jnp.float32, math.log(0.00390625), math.log(0.3))), 0.00390625, 0.3),
        "observed": normal_values(key_of[2], (STEPS, SITES), 1.0, 6.0, ((0, 32),), jnp.float32),
        "mask": with_ends((jax.random.randint(key_of[3], (STEPS, SITES), 0, 2) < 1).astype(jnp.int32), jax.random.fold_in(key_of[3], 1), 0, 1),
        "gains": draw_gains(jax.random.fold_in(key_of[7], 71), 0),
        "smooth_gains": draw_smooth_gains(jax.random.fold_in(key_of[7], 71), 0),
        "weights": draw_weights(jax.random.fold_in(key_of[7], 71), 0),
    }


HI = lax.Precision.HIGHEST


def transition(rates):
    decay = jnp.exp(-rates)
    top = jnp.concatenate([jnp.diag(decay * (1.0 + rates)), jnp.diag(decay * rates)], axis=1)
    low = jnp.concatenate([jnp.diag(-decay * rates), jnp.diag(decay * (1.0 - rates))], axis=1)
    return jnp.concatenate([top, low], axis=0)


def reference(prior_mean, rates, observed, mask, gains, smooth_gains, weights):
    trans = transition(rates)
    sites = observed.shape[1]
    seen_all = mask.astype(jnp.float32)

    def forward(carry, item):
        state, total = carry
        gain, seen, obs, weight = item
        pred = jnp.dot(trans, state, precision=HI)
        innov = seen * (obs - pred[:sites])
        state = pred + jnp.dot(gain.astype(jnp.float32), innov, precision=HI)
        quad = jnp.dot(innov, jnp.dot(weight.astype(jnp.float32), innov, precision=HI), precision=HI)
        return (state, total + quad), state

    start = (prior_mean, jnp.zeros((), jnp.float32))
    (last_state, total), filtered = lax.scan(forward, start, (gains, seen_all, observed, weights))
    count = jnp.sum(seen_all)
    fit = -0.5 * total / jnp.maximum(count, 1.0)

    def backward(later, item):
        gain, mean = item
        pred = jnp.dot(trans, mean, precision=HI)
        now = mean + jnp.dot(gain.astype(jnp.float32), later - pred, precision=HI)
        return now, now

    _, earlier = lax.scan(backward, filtered[-1], (smooth_gains[:-1], filtered[:-1]), reverse=True)
    smoothed = jnp.concatenate([earlier, filtered[-1:]], axis=0)
    return filtered, smoothed, fit
```

```python
import functools
import jax
import jax.numpy as jnp
from jax import lax
from jax.experimental import pallas as pl
from jax.experimental.pallas import tpu as pltpu
from jax.sharding import PartitionSpec as P

F32 = jnp.float32
BF16 = jnp.bfloat16
MESH = pl.DeviceIdType.MESH
PAD = 16


def split(x):
    high = x.astype(BF16)
    return high, (x - high.astype(F32)).astype(BF16)


def dot_nt(a, b):
    return lax.dot_general(a, b, (((1,), (1,)), ((), ())), preferred_element_type=F32)


def dot_nn(a, b):
    return jnp.dot(a, b, preferred_element_type=F32)


def product(a, b):
    a_high, a_low = split(a)
    b_high, b_low = split(b)
    both = jnp.concatenate([a_high, a_low], axis=1)
    twice = jnp.concatenate([b_high, b_high], axis=0)
    return dot_nn(both, twice) + dot_nn(a_high, b_low)


def column(row, state):
    return jnp.transpose(jnp.broadcast_to(row, (state, state)))


def through(col, mat):
    return jnp.sum(col * mat, axis=0, keepdims=True)


def kernel(devices, prior_ref, rates_ref, obs_ref, mask_ref, gain_ref, back_ref, weight_ref,
           filt_ref, smooth_ref, fit_ref,
           coef, obs_s, mask_s, fwd, bwd, cum, fold_f, fold_b, got_f, got_b, vec_out,
           top_out, top_in, msg, got_m, pre, suf, lead,
           fs, fr, bs, br, ms, mr, ts, tr):
    steps, sites, state = gain_ref.shape
    levels = (devices - 1).bit_length()
    me = lax.axis_index("tm")
    bits = [lax.rem(lax.div(me, 1 << k), 2) for k in range(levels)]
    peers = [me + (1 - 2 * bits[k]) * (1 << k) for k in range(levels)]

    barrier = pltpu.get_barrier_semaphore()
    everyone = [sum([(1 - 2 * bits[k]) * (1 << k) for k in range(levels) if j >> k & 1], me) for j in range(devices)]
    for j in range(1, devices):
        pl.semaphore_signal(barrier, inc=1, device_id=(everyone[j],), device_id_type=MESH)

    coef[0:1, 0:sites] = rates_ref[...]
    coef[0:1, sites:state] = rates_ref[...]
    rate = coef[0:1, :]
    lane = lax.broadcasted_iota(jnp.int32, (1, state), 1)
    sign = jnp.where(lane < sites, 1.0, -1.0).astype(F32)
    decay = jnp.exp(-rate)
    same = decay * (1.0 + sign * rate)
    cross = sign * decay * rate

    def predict(x):
        return x * same + pltpu.roll(x, sites, 1) * cross

    obs_s[...] = jnp.zeros_like(obs_s)
    mask_s[...] = jnp.zeros_like(mask_s)
    obs_s[:, 0:sites] = obs_ref[...]
    mask_s[:, 0:sites] = mask_ref[...].astype(F32)

    last = jnp.where(me == devices - 1, 0.0, 1.0).astype(F32)

    def back_twin(t):
        j = back_ref[t]
        if t == steps - 1:
            j = (j.astype(F32) * last).astype(BF16)
        return jnp.concatenate([j, j], axis=1)

    rows = state + PAD
    row = lax.broadcasted_iota(jnp.int32, (rows, state), 0)
    col = lax.broadcasted_iota(jnp.int32, (rows, state), 1)
    is_off = row >= state
    x = jnp.where(row == col, 1.0, 0.0).astype(F32)
    eye = x
    y = x[:state]
    for i in range(steps):
        pred = predict(x)
        seen = mask_s[i:i + 1, :] * (jnp.where(is_off, obs_s[i:i + 1, :], 0.0) - pred)
        high = seen.astype(BF16).astype(F32)
        pair = high + pltpu.roll(seen - high, sites, 1)
        x = pred + dot_nn(pair.astype(BF16), jnp.concatenate([gain_ref[i], gain_ref[i]], axis=0))
        fwd[i] = x
        t = steps - 1 - i
        high, low = split(y)
        y = dot_nt(jnp.concatenate([high, low], axis=1), back_twin(t))
        bwd[t] = y

    def remote(src, dst, send, recv, k):
        return pltpu.make_async_remote_copy(src_ref=src, dst_ref=dst, send_sem=send.at[k], recv_sem=recv.at[k],
                                            device_id=(peers[k],), device_id_type=MESH)

    pl.semaphore_wait(barrier, devices - 1)
    copies = []
    f_copy = remote(fwd.at[steps - 1], got_f.at[0], fs, fr, 0)
    f_copy.start()
    b_copy = remote(bwd.at[0], got_b.at[0], bs, br, 0)
    b_copy.start()
    copies += [f_copy, b_copy]

    u = jnp.zeros((rows, state), F32)
    t_next = steps - 1
    share = -(-steps // (levels - 1))
    f_tot, b_tot = x, y
    for k in range(levels - 1):
        for _ in range(share):
            if t_next >= 0:
                t = t_next
                here = fwd[t]
                high, low = split(u - predict(here))
                u = here + dot_nt(jnp.concatenate([high, low], axis=1), back_twin(t))
                cum[t] = u
                t_next -= 1
        late = bits[k] == 1
        f_copy.wait_recv()
        other = got_f[k]
        first = jnp.where(late, other, f_tot)
        second = jnp.where(late, f_tot, other)
        f_tot = product(first, second[:state]) + jnp.where(is_off, second[state:state + 1], 0.0)
        if k + 1 < levels - 1:
            fold_f[k] = f_tot
            f_copy = remote(fold_f.at[k], got_f.at[k + 1], fs, fr, k + 1)
            f_copy.start()
            copies.append(f_copy)
        else:
            half = through(column(prior_ref[...], state), f_tot[:state]) + f_tot[state:state + 1]
            top_out[...] = jnp.broadcast_to(half, top_out.shape)
            top_copy = pltpu.make_async_remote_copy(
                src_ref=top_out, dst_ref=top_in, send_sem=ts.at[0], recv_sem=tr.at[0],
                device_id=(peers[k + 1],), device_id_type=MESH)
            top_copy.start()
            copies.append(top_copy)
        if k == 0:
            pre[...] = jnp.where(late, other, eye)
        else:
            held = pre[...]
            moved = product(other, held[:state]) + jnp.where(is_off, held[state:state + 1], 0.0)
            pre[...] = jnp.where(late, moved, held)
        b_copy.wait_recv()
        other_b = got_b[k]
        if k + 1 < levels - 1:
            b_tot = product(jnp.where(late, b_tot, other_b), jnp.where(late, other_b, b_tot))
            fold_b[k] = b_tot
            b_copy = remote(fold_b.at[k], got_b.at[k + 1], bs, br, k + 1)
            b_copy.start()
            copies.append(b_copy)
        if k == 0:
            suf[1] = jnp.where(late, eye[:state], other_b)
            lead[1] = jnp.where(late, other_b, eye[:state])
        else:
            joined = product(jnp.where(late, lead[k], other_b), jnp.where(late, other_b, suf[k]))
            suf[k + 1] = jnp.where(late, suf[k], joined)
            lead[k + 1] = jnp.where(late, joined, lead[k])

    top_copy.wait_recv()
    m = jnp.where(bits[levels - 1] == 1, top_in[0:1, :], prior_ref[...])
    m = through(column(m, state), pre[0:state, :]) + pre[state:state + 1, :]

    m_col = column(m, state)
    g = through(m_col, cum[0, 0:state, :]) + cum[0, state:state + 1, :]

    vec_out[0:1, :] = m
    for t in range(steps):
        now = through(m_col, fwd[t, 0:state, :]) + fwd[t, state:state + 1, :]
        filt_ref[t:t + 1, :] = now
        vec_out[t + 1:t + 2, :] = now

    v = mask_s[...] * (obs_s[...] - predict(vec_out[0:steps, :]))
    v_rows = lax.broadcasted_iota(jnp.int32, v.shape, 0)
    acc = jnp.zeros((2 * steps, sites), F32)
    for t in range(steps):
        high, low = split(jnp.where(v_rows == t, v, 0.0))
        acc += dot_nn(jnp.concatenate([high, low], axis=0)[:, 0:sites], weight_ref[t])
    quad = jnp.sum(v[:, 0:sites] * (acc[0:steps] + acc[steps:]), axis=0, keepdims=True)
    q_tot = jnp.sum(quad, axis=1, keepdims=True)
    c_tot = jnp.sum(jnp.sum(mask_s[...], axis=0, keepdims=True), axis=1, keepdims=True)
    g_col = column(g, state)
    for k in range(levels):
        msg[k, 0:1, :] = g if k == 0 else through(g_col, lead[k])
        msg[k, 1:2, :] = jnp.broadcast_to(q_tot, (1, state))
        msg[k, 2:3, :] = jnp.broadcast_to(c_tot, (1, state))
        msg[k, 3:8, :] = jnp.zeros((5, state), F32)
    arrivals = []
    for j in reversed(range(1, devices)):
        copy = pltpu.make_async_remote_copy(
            src_ref=msg.at[j.bit_length() - 1], dst_ref=got_m.at[j], send_sem=ms.at[j], recv_sem=mr.at[j],
            device_id=(everyone[j],), device_id_type=MESH)
        copy.start()
        arrivals.append((j, copy))
        copies.append(copy)
    for t in range(steps):
        smooth_ref[t:t + 1, :] = through(m_col, cum[t, 0:state, :]) + cum[t, state:state + 1, :]
    sums = [jnp.zeros((8, state), F32) for _ in range(levels)]
    for j, copy in reversed(arrivals):
        copy.wait_recv()
        sums[j.bit_length() - 1] += got_m[j]
    h = jnp.where(bits[0] == 1, 0.0, sums[0][0:1])
    for k in range(1, levels):
        h += through(column(jnp.where(bits[k] == 1, 0.0, sums[k][0:1]), state), suf[k])
    s_col = column(h, state)
    for t in range(steps):
        smooth_ref[t:t + 1, :] = smooth_ref[t:t + 1, :] + through(s_col, bwd[t])
    whole = functools.reduce(jnp.add, sums)
    q_tot = q_tot + whole[1:2, 0:1]
    c_tot = c_tot + whole[2:3, 0:1]
    fit_ref[...] = jnp.broadcast_to(-0.5 * q_tot / jnp.maximum(c_tot, 1.0), fit_ref.shape)
    for c in copies:
        c.wait_send()


def finish(a_ref, b_ref, c_ref, x_ref, y_ref, z_ref):
    x_ref[...] = a_ref[...]
    y_ref[...] = b_ref[...]
    z_ref[...] = c_ref[0:1, 0:1]


def body(devices, prior_mean, rates, observed, mask, gains, smooth_gains, weights):
    steps, state, sites = gains.shape
    levels = (devices - 1).bit_length()
    rows = state + PAD
    vmem = pl.BlockSpec(memory_space=pltpu.VMEM)
    dma = pltpu.SemaphoreType.DMA
    filtered, smoothed, fit = pl.pallas_call(
        functools.partial(kernel, devices),
        out_shape=(pltpu.VMEM((steps, state), F32), pltpu.VMEM((steps, state), F32),
                   pltpu.VMEM((8, state), F32)),
        in_specs=[vmem] * 7,
        out_specs=(vmem, vmem, vmem),
        scratch_shapes=[
            pltpu.VMEM((8, state), F32),
            pltpu.VMEM((steps, state), F32),
            pltpu.VMEM((steps, state), F32),
            pltpu.VMEM((steps, rows, state), F32),
            pltpu.VMEM((steps, state, state), F32),
            pltpu.VMEM((steps, rows, state), F32),
            pltpu.VMEM((levels, rows, state), F32),
            pltpu.VMEM((levels, state, state), F32),
            pltpu.VMEM((levels, rows, state), F32),
            pltpu.VMEM((levels, state, state), F32),
            pltpu.VMEM((steps + 8, state), F32),
            pltpu.VMEM((8, state), F32),
            pltpu.VMEM((8, state), F32),
            pltpu.VMEM((levels, 8, state), F32),
            pltpu.VMEM((devices, 8, state), F32),
            pltpu.VMEM((rows, state), F32),
            pltpu.VMEM((levels, state, state), F32),
            pltpu.VMEM((levels, state, state), F32),
            dma((levels,)), dma((levels,)), dma((levels,)), dma((levels,)),
            dma((devices,)), dma((devices,)), dma((1,)), dma((1,)),
        ],
        compiler_params=pltpu.CompilerParams(collective_id=0, has_side_effects=True),
        name="smoother",
    )(prior_mean.reshape(1, state), rates.reshape(1, sites), observed, mask, jnp.swapaxes(gains, 1, 2), smooth_gains, weights)
    filtered, smoothed, fit = pl.pallas_call(
        finish,
        out_shape=(jax.ShapeDtypeStruct((steps, state), F32), jax.ShapeDtypeStruct((steps, state), F32),
                   jax.ShapeDtypeStruct((1, 1), F32)),
        in_specs=[vmem] * 3,
        out_specs=(vmem, vmem, vmem),
        name="finish",
    )(*[pltpu.with_memory_space_constraint(a, pltpu.VMEM) for a in (filtered, smoothed, fit)])
    return filtered, smoothed, fit.reshape(())


def solution(mesh):
    placed = (P(), P(), P("tm", None), P("tm", None), P("tm", None, None), P("tm", None, None), P("tm", None, None))
    return jax.shard_map(
        functools.partial(body, mesh.shape["tm"]),
        mesh=mesh,
        in_specs=placed,
        out_specs=(P("tm", None), P("tm", None), P()),
        check_vma=False,
    )
```
